512 devices in a mesh: unit: 2 (over y_1), row: 16 (over y_0, x, core), col: 16 (over z, y_2).
Axes of the slice: x: 4, y: 8 (y_0: 2, y_1: 2, y_2: 2; y = y_0 * 4 + y_1 * 2 + y_2), z: 8, core: 2. Of those that a mesh axis runs over, the one named last changes fastest.
Arguments:
- tracer: float32 [4, 128, 256, 256], P('unit', None, 'row', 'col'), parts along dimension 0, may hold values from -6 to 6
- symbol_x: float32 [128], replicated, may hold values from 0.3 to 3
- symbol_y: float32 [256], replicated, may hold values from 0.3 to 3
- symbol_z: float32 [256], replicated, may hold values from 0.3 to 3
Outputs:
- smoothed: float32 [4, 128, 256, 256], P('unit', None, 'row', 'col'), parts along dimension 0
The draws below stay inside these ranges and needn't reach their ends.
There are 2 independent parts, one for each index of `unit`. The reference program is written for one: setup_inputs(seed, part) draws one part's arguments, and reference() takes and returns one part's arrays. A program takes and returns all parts, laid end to end along the dimension named above; an argument that names none is the same for every part. Nothing has to cross between parts.
All inputs are finite; a program needn't handle non-finite values.
Results may differ from the reference program's by a relative error of at most 0.0003.
Values sent between devices are 32-bit elements.
A program may use at most 64 MiB of HBM per device.

```python
import jax
import jax.numpy as jnp
from jax import lax

GRID_X = 128
GRID_Y = 256
GRID_Z = 256
FIELDS = 2


def levels(stream_key, extent, shards, smallest, top_value):
    def one(dim, shards_of):
        steps = jax.random.uniform(jax.random.fold_in(jax.random.fold_in(stream_key, 6), dim), (shards_of,), jnp.float32, smallest / len(shards), top_value / len(shards))
        return jnp.repeat(jnp.exp(steps), extent[dim] // shards_of).reshape((-1,) + (1,) * (len(extent) - dim - 1))

    factor_of = one(*shards[0])
    for cut in shards[1:]:
        factor_of = factor_of * one(*cut)
    return factor_of


def noise(key, extent, deviation, bound, split=(), dtype=jnp.bfloat16):
    level = levels(key, extent, split, -0.22, 0.18) if split else 1.0
    drawn = jax.random.normal(key, extent, jnp.float32) * deviation * level
    return jnp.minimum(jnp.maximum(drawn, -bound), bound).astype(dtype)


def setup_inputs(seed: int = 0, part: int = 0) -> dict:
    arg_keys = jax.random.split(jax.random.key(seed), 5)
    part_keys = jax.random.split(jax.random.fold_in(arg_keys[4], part), 5)
    return {
        "tracer": noise(part_keys[0], (FIELDS, GRID_X, GRID_Y, GRID_Z), 1.0, 6.0, ((2, 16), (3, 16)), jnp.float32),
        "symbol_x": jnp.clip(jax.random.uniform(arg_keys[1], (GRID_X,), jnp.float32, 0.3, 3.0), 0.3, 3.0),
        "symbol_y": jnp.clip(jax.random.uniform(arg_keys[2], (GRID_Y,), jnp.float32, 0.3, 3.0), 0.3, 3.0),
        "symbol_z": jnp.clip(jax.random.uniform(arg_keys[3], (GRID_Z,), jnp.float32, 0.3, 3.0), 0.3, 3.0),
    }


def mode_table(count):
    rank = jnp.arange(count)
    angle = jnp.pi / (4 * count) * ((2 * rank[:, None] + 1) * (2 * rank[None, :] + 1) % (8 * count)).astype(jnp.float32)
    return jnp.cos(angle) * (2.0 / count) ** 0.5

def to_modes(values, dim):
    moved = jnp.tensordot(values, mode_table(values.shape[dim]), axes=([dim], [0]), precision=lax.Precision.HIGHEST)
    return jnp.moveaxis(moved, -1, dim)

def reference(tracer, symbol_x, symbol_y, symbol_z):
    modes = tracer
    modes = to_modes(modes, 1)
    modes = to_modes(modes, 2)
    modes = to_modes(modes, 3)
    symbol = symbol_x[:, None, None] + symbol_y[None, :, None] + symbol_z[None, None, :]
    modes = modes * lax.rsqrt(symbol)
    smoothed = modes
    smoothed = to_modes(smoothed, 3)
    smoothed = to_modes(smoothed, 2)
    smoothed = to_modes(smoothed, 1)
    return smoothed
```

```python
import functools

import jax
import jax.numpy as jnp
import numpy as np
from jax import lax
from jax.experimental import pallas as pl
from jax.experimental.pallas import tpu as pltpu
from jax.sharding import PartitionSpec as P

MESH = pl.DeviceIdType.MESH
F32, BF16 = jnp.float32, jnp.bfloat16


def mode_table(count):
    rank = np.arange(count)
    angle = np.pi / (4 * count) * ((2 * rank[:, None] + 1) * (2 * rank[None, :] + 1) % (8 * count))
    table = (np.cos(angle) * np.sqrt(2.0 / count)).astype(np.float32)
    high = table.astype(jnp.bfloat16)
    low = (table - high.astype(np.float32)).astype(jnp.bfloat16)
    return np.stack([high, low])


def split(values):
    high = values.astype(BF16)
    return high, (values - high.astype(F32)).astype(BF16)


def dot(a, b, dims):
    out = None
    for i, j in ((0, 1), (1, 0), (0, 0)):
        term = lax.dot_general(a[i], b[j], (dims, ((), ())), preferred_element_type=F32)
        out = term if out is None else out + term
    return out


NN, NT, TN = ((1,), (0,)), ((1,), (1,)), ((0,), (0,))


def exchanged(tiles):
    tiles = pltpu.roll(tiles, 0, 2, stride=16, stride_axis=1)
    group = lax.broadcasted_iota(jnp.int32, tiles.shape, 2) // 16
    for bit, step in ((1, 7), (2, 6), (4, 4)):
        tiles = jnp.where(group // bit % 2 == 1, pltpu.roll(tiles, step, 1), tiles)
    return pltpu.roll(tiles, 0, 2, stride=16, stride_axis=1)


def kernel(a_ref, hx_ref, h_ref, hb_ref, sx_ref, sy_ref, sz_ref, out_ref,
           send1, recv1, recv2, send3, recv3, recv4, send_sem, recv_sem, own_sem):
    r, c = lax.axis_index("row"), lax.axis_index("col")
    barrier = pltpu.get_barrier_semaphore()

    @pl.loop(1, 16)
    def _(i):
        pl.semaphore_signal(barrier, inc=1, device_id={"row": (r + i) % 16}, device_id_type=MESH)
        pl.semaphore_signal(barrier, inc=1, device_id={"col": (c + i) % 16}, device_id_type=MESH)

    def slot(col):
        return col // 8 * 8 + (8 - col % 8) % 8

    def refs(k, h, mine, t):
        if k == 0:
            return send1.at[h, t], recv1.at[h, mine]
        if k == 1:
            return recv1.at[h, :, pl.ds(t, 1)], recv2.at[h, :, pl.ds(mine, 1)]
        if k == 2:
            return send3.at[h, :, pl.ds(slot(t), 1)], recv3.at[h, :, pl.ds(mine, 1)]
        return recv3.at[h, t], recv4.at[h, mine]

    def start(k, h):
        axis, mine = ("row", r) if k in (0, 3) else ("col", c)

        @pl.loop(1, 16)
        def _(i):
            t = (mine + i) % 16
            src, dst = refs(k, h, mine, t)
            pltpu.make_async_remote_copy(src, dst, send_sem.at[k, h], recv_sem.at[k, h],
                                         device_id={axis: t}, device_id_type=MESH).start()
        src, dst = refs(k, h, mine, mine)
        pltpu.make_async_copy(src, dst, own_sem.at[k, h]).start()

    def finish(k, h):
        axis, mine = ("row", r) if k in (0, 3) else ("col", c)
        src, dst = refs(k, h, mine, mine)
        pltpu.make_async_copy(src, dst, own_sem.at[k, h]).wait()
        part = send1.at[h, pl.ds(0, 15)]
        pltpu.make_async_copy(part, part, recv_sem.at[k, h]).wait()

    def sent(k, h):
        part = send1.at[h, pl.ds(0, 15)]
        pltpu.make_async_copy(part, part, send_sem.at[k, h]).wait()

    hx = hx_ref[0], hx_ref[1]
    table = h_ref[0], h_ref[1]
    backwards = hb_ref[0], hb_ref[1]
    for f in range(2):
        for h in range(2):
            rows = split(a_ref[f, pl.ds(8 * h, 8)].reshape(128, 128))
            send1[h, pl.ds(8 * f, 8)] = dot(hx, rows, NT).reshape(8, 16, 128)
    pl.semaphore_wait(barrier, 30)
    for h in range(2):
        start(0, h)

    symbol_y = jnp.broadcast_to(sy_ref[...], (256, 256)).T
    symbol = sx_ref[r % 8 * 16 + c] + symbol_y + sz_ref[...]
    scale = lax.rsqrt(symbol)

    for h in range(2):
        finish(0, h)
        start(1, h)
    for h in range(2):
        finish(1, h)

    tiles = exchanged(recv2[...].reshape(64, 8, 128)).reshape(2, 16, 2, 8, 128)
    plane = jnp.concatenate(
        [jnp.stack([tiles[0, :, g], tiles[1, :, g]], axis=1).reshape(256, 128) for g in range(2)], axis=1
    )
    plane = dot(split(plane), table, NN)
    plane = dot(backwards, split(plane), NN) * scale
    plane = dot(table, split(plane), NN)
    plane = dot(split(plane), table, NN).reshape(16, 2, 8, 256)
    for h in range(2):
        part = jnp.stack([plane[:, h, :, :128], plane[:, h, :, 128:]], axis=1).reshape(32, 8, 128)
        send3[h] = exchanged(part).reshape(16, 16, 128)
        start(2, h)
    for h in range(2):
        finish(2, h)
        start(3, h)
    for h in range(2):
        finish(3, h)
        for f in range(2):
            rows = split(recv4[h, pl.ds(8 * f, 8)].reshape(128, 128))
            out_ref[f, pl.ds(8 * h, 8)] = dot(rows, hx, TN).reshape(8, 16, 128)
    for k in range(4):
        for h in range(2):
            sent(k, h)


def shards(tracer, symbol_x, symbol_y, symbol_z):
    values = jnp.transpose(tracer, (0, 2, 3, 1))
    vmem, smem = pl.BlockSpec(memory_space=pltpu.VMEM), pl.BlockSpec(memory_space=pltpu.SMEM)
    table, place = mode_table(256), np.arange(256)
    backwards = place // 8 * 8 + -place % 8
    block = pltpu.VMEM((2, 16, 16, 128), F32)
    out = pl.pallas_call(
        kernel,
        out_shape=jax.ShapeDtypeStruct(values.shape, F32),
        in_specs=[vmem, vmem, vmem, vmem, smem, vmem, vmem],
        out_specs=vmem,
        scratch_shapes=[block] * 6 + [pltpu.SemaphoreType.DMA((4, 2))] * 3,
        compiler_params=pltpu.CompilerParams(collective_id=0, has_side_effects=True),
    )(values, jnp.asarray(mode_table(128)), jnp.asarray(table), jnp.asarray(table[:, :, backwards]),
      symbol_x, symbol_y.reshape(1, 256), symbol_z.reshape(1, 256))
    return jnp.transpose(out, (0, 3, 1, 2))


def solution(mesh):
    in_specs = (P("unit", None, "row", "col"), P(), P(), P())
    out_specs = P("unit", None, "row", "col")
    return jax.shard_map(shards, mesh=mesh, in_specs=in_specs, out_specs=out_specs, check_vma=False)
```

```python
import functools

import jax
import jax.numpy as jnp
import numpy as np
from jax import lax
from jax.experimental import pallas as pl
from jax.experimental.pallas import tpu as pltpu
from jax.sharding import PartitionSpec as P

MESH = pl.DeviceIdType.MESH
OUT = (1, 0), (0, 0), (0, 1), (1, 1)
OUT_NEXT = (0, 0), (0, 1), (1, 0), (1, 1)
BACK = (1, 0), (1, 1), (0, 0), (0, 1)
F32, BF16 = jnp.float32, jnp.bfloat16


def mode_table(count):
    rank = np.arange(count)
    angle = np.pi / (4 * count) * ((2 * rank[:, None] + 1) * (2 * rank[None, :] + 1) % (8 * count))
    table = (np.cos(angle) * np.sqrt(2.0 / count)).astype(np.float32)
    high = table.astype(jnp.bfloat16)
    low = (table - high.astype(np.float32)).astype(jnp.bfloat16)
    return np.stack([high, low])


def split(values):
    high = values.astype(BF16)
    return high, (values - high.astype(F32)).astype(BF16)


def dot(a, b, dims):
    out = None
    for i, j in ((0, 1), (1, 0), (0, 0)):
        term = lax.dot_general(a[i], b[j], (dims, ((), ())), preferred_element_type=F32)
        out = term if out is None else out + term
    return out


NN, NT, TN = ((1,), (0,)), ((1,), (1,)), ((0,), (0,))


def exchanged(tiles):
    tiles = pltpu.roll(tiles, 0, 2, stride=16, stride_axis=1)
    group = lax.broadcasted_iota(jnp.int32, tiles.shape, 2) // 16
    for bit, step in ((1, 7), (2, 6), (4, 4)):
        tiles = jnp.where(group // bit % 2 == 1, pltpu.roll(tiles, step, 1), tiles)
    return pltpu.roll(tiles, 0, 2, stride=16, stride_axis=1)


def kernel(a_ref, hx_ref, h_ref, hb_ref, sx_ref, sy_ref, sz_ref, out_ref,
           send1, recv1, recv2, send3, recv3, recv4, send_sem, recv_sem, own_sem):
    r, c = lax.axis_index("row"), lax.axis_index("col")
    barrier = pltpu.get_barrier_semaphore()

    @pl.loop(1, 16)
    def _(i):
        pl.semaphore_signal(barrier, inc=1, device_id={"row": (r + i) % 16}, device_id_type=MESH)
        pl.semaphore_signal(barrier, inc=1, device_id={"col": (c + i) % 16}, device_id_type=MESH)

    def slot(col):
        return col // 8 * 8 + (8 - col % 8) % 8

    half = r // 8
    near, far = half * 8, (1 - half) * 8

    def refs(k, h, base, mine, t):
        if k == 0:
            return send1.at[h, t], recv1.at[h, mine]
        if k == 1:
            return recv1.at[h, pl.ds(base, 8), pl.ds(t, 1)], recv2.at[h, pl.ds(base, 8), pl.ds(mine, 1)]
        if k == 2:
            return send3.at[h, pl.ds(base, 8), pl.ds(slot(t), 1)], recv3.at[h, pl.ds(base, 8), pl.ds(mine, 1)]
        return recv3.at[h, t], recv4.at[h, mine]

    def own(k, h, side):
        return pltpu.make_async_copy(*refs(k, h, (near, far)[side], *((r, r) if k in (0, 3) else (c, c))),
                                     own_sem.at[k, side, h])

    def start(k, side, h):
        base, rows = (near, far)[side], k in (0, 3)
        axis, mine = ("row", r) if rows else ("col", c)

        @pl.loop(0 if rows and side else 1, 8 if rows else 16)
        def _(i):
            t = base + (r + i) % 8 if rows else (c + i) % 16
            src, dst = refs(k, h, base, mine, t)
            pltpu.make_async_remote_copy(src, dst, send_sem.at[k, side, h], recv_sem.at[k, side, h],
                                         device_id={axis: t}, device_id_type=MESH).start()
        if not (rows and side):
            own(k, h, side).start()

    def await_all(k, side, h, sem):
        part = send1.at[h, pl.ds(0, 7 + side)] if k in (0, 3) else send1.at[h, pl.ds(0, 15), pl.ds(0, 8)]
        pltpu.make_async_copy(part, part, sem.at[k, side, h]).wait()

    def finish(k, side, h):
        if k in (1, 2) or not side:
            own(k, h, side).wait()
        await_all(k, side, h, recv_sem)

    hx = hx_ref[0], hx_ref[1]
    table = h_ref[0], h_ref[1]
    backwards = hb_ref[0], hb_ref[1]
    for f in range(2):
        for h in range(2):
            rows = split(a_ref[f, pl.ds(8 * h, 8)].reshape(128, 128))
            send1[h, pl.ds(8 * f, 8)] = dot(hx, rows, NT).reshape(8, 16, 128)
    pl.semaphore_wait(barrier, 30)
    for side, h in OUT:
        start(0, side, h)

    symbol_y = jnp.broadcast_to(sy_ref[...], (256, 256)).T
    symbol = sx_ref[r % 8 * 16 + c] + symbol_y + sz_ref[...]
    scale = lax.rsqrt(symbol)

    for side, h in OUT_NEXT:
        finish(0, side, h)
        start(1, side, h)
    for side, h in OUT_NEXT:
        finish(1, side, h)

    tiles = exchanged(recv2[...].reshape(64, 8, 128)).reshape(2, 16, 2, 8, 128)
    plane = jnp.concatenate(
        [jnp.stack([tiles[0, :, g], tiles[1, :, g]], axis=1).reshape(256, 128) for g in range(2)], axis=1
    )
    plane = dot(split(plane), table, NN)
    plane = dot(backwards, split(plane), NN) * scale
    plane = dot(table, split(plane), NN)
    plane = dot(split(plane), table, NN).reshape(16, 2, 8, 256)
    for h in range(2):
        part = jnp.stack([plane[:, h, :, :128], plane[:, h, :, 128:]], axis=1).reshape(32, 8, 128)
        send3[h] = exchanged(part).reshape(16, 16, 128)
    for side, h in BACK:
        start(2, side, h)
    for side, h in BACK:
        finish(2, side, h)
        start(3, side, h)
    for side, h in BACK:
        finish(3, side, h)
        f = (half, 1 - half)[side]
        rows = split(recv4[h, pl.ds(8 * f, 8)].reshape(128, 128))
        out_ref[f, pl.ds(8 * h, 8)] = dot(rows, hx, TN).reshape(8, 16, 128)
    for k in range(4):
        for side, h in OUT:
            await_all(k, side, h, send_sem)


def shards(tracer, symbol_x, symbol_y, symbol_z):
    values = jnp.transpose(tracer, (0, 2, 3, 1))
    vmem, smem = pl.BlockSpec(memory_space=pltpu.VMEM), pl.BlockSpec(memory_space=pltpu.SMEM)
    table, place = mode_table(256), np.arange(256)
    backwards = place // 8 * 8 + -place % 8
    block = pltpu.VMEM((2, 16, 16, 128), F32)
    out = pl.pallas_call(
        kernel,
        out_shape=jax.ShapeDtypeStruct(values.shape, F32),
        in_specs=[vmem, vmem, vmem, vmem, smem, vmem, vmem],
        out_specs=vmem,
        scratch_shapes=[block] * 6 + [pltpu.SemaphoreType.DMA((4, 2, 2))] * 3,
        compiler_params=pltpu.CompilerParams(collective_id=0, has_side_effects=True),
    )(values, jnp.asarray(mode_table(128)), jnp.asarray(table), jnp.asarray(table[:, :, backwards]),
      symbol_x, symbol_y.reshape(1, 256), symbol_z.reshape(1, 256))
    return jnp.transpose(out, (0, 3, 1, 2))


def solution(mesh):
    in_specs = (P("unit", None, "row", "col"), P(), P(), P())
    out_specs = P("unit", None, "row", "col")
    return jax.shard_map(shards, mesh=mesh, in_specs=in_specs, out_specs=out_specs, check_vma=False)
```

```python
import functools

import jax
import jax.numpy as jnp
import numpy as np
from jax import lax
from jax.experimental import pallas as pl
from jax.experimental.pallas import tpu as pltpu
from jax.sharding import PartitionSpec as P

MESH = pl.DeviceIdType.MESH
OUT = (1, 0), (0, 0), (0, 1), (1, 1)
OUT_NEXT = (0, 0), (0, 1), (1, 0), (1, 1)
BACK = (1, 0), (1, 1), (0, 0), (0, 1)
F32, BF16 = jnp.float32, jnp.bfloat16


def mode_table(count):
    rank = np.arange(count)
    angle = np.pi / (4 * count) * ((2 * rank[:, None] + 1) * (2 * rank[None, :] + 1) % (8 * count))
    table = (np.cos(angle) * np.sqrt(2.0 / count)).astype(np.float32)
    high = table.astype(jnp.bfloat16)
    low = (table - high.astype(np.float32)).astype(jnp.bfloat16)
    return np.stack([high, low])


def split(values):
    high = values.astype(BF16)
    return high, (values - high.astype(F32)).astype(BF16)


def dot(a, b, dims):
    out = None
    for i, j in ((0, 1), (1, 0), (0, 0)):
        term = lax.dot_general(a[i], b[j], (dims, ((), ())), preferred_element_type=F32)
        out = term if out is None else out + term
    return out


NN, NT, TN = ((1,), (0,)), ((1,), (1,)), ((0,), (0,))


def exchanged(tiles):
    tiles = pltpu.roll(tiles, 0, 2, stride=16, stride_axis=1)
    group = lax.broadcasted_iota(jnp.int32, tiles.shape, 2) // 16
    for bit, step in ((1, 7), (2, 6), (4, 4)):
        tiles = jnp.where(group // bit % 2 == 1, pltpu.roll(tiles, step, 1), tiles)
    return pltpu.roll(tiles, 0, 2, stride=16, stride_axis=1)


def kernel(a_ref, hx_ref, h_ref, hb_ref, hc_ref, sx_ref, sy_ref, sz_ref, out_ref,
           send1, recv1, recv2, send3, recv3, recv4, send_sem, recv_sem, own_sem):
    r, c = lax.axis_index("row"), lax.axis_index("col")
    a = r % 8 * 2 + c % 2
    b = r // 8 * 8 + c // 2

    def at_a(t):
        return {"row": b // 8 * 8 + t // 2, "col": b % 8 * 2 + t % 2}

    def at_b(t):
        return {"row": t // 8 * 8 + a // 2, "col": t % 8 * 2 + a % 2}

    barrier = pltpu.get_barrier_semaphore()

    @pl.loop(1, 16)
    def _(i):
        pl.semaphore_signal(barrier, inc=1, device_id=at_a((a + i) % 16), device_id_type=MESH)
        pl.semaphore_signal(barrier, inc=1, device_id=at_b((b + i) % 16), device_id_type=MESH)

    def slot(col):
        return col // 8 * 8 + (8 - col % 8) % 8

    half = a // 8
    near, far = half * 8, (1 - half) * 8

    def refs(k, h, base, mine, t):
        if k == 0:
            return send1.at[h, t], recv1.at[h, mine]
        if k == 1:
            return recv1.at[h, pl.ds(base, 8), pl.ds(t, 1)], recv2.at[h, pl.ds(base, 8), pl.ds(mine, 1)]
        if k == 2:
            return send3.at[h, pl.ds(base, 8), pl.ds(slot(t), 1)], recv3.at[h, pl.ds(base, 8), pl.ds(mine, 1)]
        return recv3.at[h, t], recv4.at[h, mine]

    def own(k, h, side):
        return pltpu.make_async_copy(*refs(k, h, (near, far)[side], *((a, a) if k in (0, 3) else (b, b))),
                                     own_sem.at[k, side, h])

    def start(k, side, h):
        base, rows = (near, far)[side], k in (0, 3)
        mine, at = (a, at_a) if rows else (b, at_b)

        @pl.loop(0 if rows and side else 1, 8 if rows else 16)
        def _(i):
            t = base + (a + i) % 8 if rows else (b + i) % 16
            src, dst = refs(k, h, base, mine, t)
            pltpu.make_async_remote_copy(src, dst, send_sem.at[k, side, h], recv_sem.at[k, side, h],
                                         device_id=at(t), device_id_type=MESH).start()
        if not (rows and side):
            own(k, h, side).start()

    def await_all(k, side, h, sem):
        part = send1.at[h, pl.ds(0, 7 + side)] if k in (0, 3) else send1.at[h, pl.ds(0, 15), pl.ds(0, 8)]
        pltpu.make_async_copy(part, part, sem.at[k, side, h]).wait()

    def finish(k, side, h):
        if k in (1, 2) or not side:
            own(k, h, side).wait()
        await_all(k, side, h, recv_sem)

    hx = hx_ref[0], hx_ref[1]
    table = h_ref[0], h_ref[1]
    backwards = hb_ref[0], hb_ref[1]
    columns = hc_ref[0], hc_ref[1]
    for f in range(2):
        for h in range(2):
            rows = split(a_ref[f, pl.ds(8 * h, 8)].reshape(128, 128))
            send1[h, pl.ds(8 * f, 8)] = dot(hx, rows, NT).reshape(8, 16, 128)
    pl.semaphore_wait(barrier, 30)
    for side, h in OUT:
        start(0, side, h)

    symbol_y = jnp.broadcast_to(sy_ref[...], (256, 256)).T
    symbol = sx_ref[a % 8 * 16 + b] + symbol_y + sz_ref[...]
    scale = lax.rsqrt(symbol)

    for side, h in OUT_NEXT:
        finish(0, side, h)
        start(1, side, h)
    for side, h in OUT_NEXT:
        finish(1, side, h)

    tiles = exchanged(recv2[...].reshape(64, 8, 128)).reshape(2, 8, 2, 2, 8, 128)
    plane = jnp.concatenate(
        [jnp.stack([jnp.stack([tiles[h, :, g, y] for h in range(2)], axis=1) for y in range(2)]).reshape(256, 128)
         for g in range(2)], axis=1
    )
    plane = dot(split(plane), columns, NN)
    plane = dot(backwards, split(plane), NN) * scale
    plane = dot(table, split(plane), NN)
    plane = dot(split(plane), columns, NT).reshape(2, 8, 2, 8, 256)
    for h in range(2):
        part = jnp.stack(
            [jnp.stack([plane[y, :, h, :, 128 * g:128 * (g + 1)] for y in range(2)], axis=1) for g in range(2)], axis=1
        ).reshape(32, 8, 128)
        send3[h] = exchanged(part).reshape(16, 16, 128)
    for side, h in BACK:
        start(2, side, h)
    for side, h in BACK:
        finish(2, side, h)
        start(3, side, h)
    for side, h in BACK:
        finish(3, side, h)
        f = (half, 1 - half)[side]
        rows = split(recv4[h, pl.ds(8 * f, 8)].reshape(128, 128))
        out_ref[f, pl.ds(8 * h, 8)] = dot(rows, hx, TN).reshape(8, 16, 128)
    for k in range(4):
        for side, h in OUT:
            await_all(k, side, h, send_sem)


def shards(tracer, symbol_x, symbol_y, symbol_z):
    values = jnp.transpose(tracer, (0, 2, 3, 1))
    vmem, smem = pl.BlockSpec(memory_space=pltpu.VMEM), pl.BlockSpec(memory_space=pltpu.SMEM)
    table, place = mode_table(256), np.arange(256)
    backwards = place // 8 * 8 + -place % 8
    apart = (place % 128 // 16 * 2 + place // 128) * 16 + place % 16
    block = pltpu.VMEM((2, 16, 16, 128), F32)
    out = pl.pallas_call(
        kernel,
        out_shape=jax.ShapeDtypeStruct(values.shape, F32),
        in_specs=[vmem, vmem, vmem, vmem, vmem, smem, vmem, vmem],
        out_specs=vmem,
        scratch_shapes=[block] * 6 + [pltpu.SemaphoreType.DMA((4, 2, 2))] * 3,
        compiler_params=pltpu.CompilerParams(collective_id=0, has_side_effects=True),
    )(values, jnp.asarray(mode_table(128)), jnp.asarray(table), jnp.asarray(table[:, :, backwards]),
      jnp.asarray(table[:, apart]),
      symbol_x, symbol_y.reshape(1, 256), symbol_z.reshape(1, 256))
    return jnp.transpose(out, (0, 3, 1, 2))


def solution(mesh):
    in_specs = (P("unit", None, "row", "col"), P(), P(), P())
    out_specs = P("unit", None, "row", "col")
    return jax.shard_map(shards, mesh=mesh, in_specs=in_specs, out_specs=out_specs, check_vma=False)
```

```python
import functools

import jax
import jax.numpy as jnp
import numpy as np
from jax import lax
from jax.experimental import pallas as pl
from jax.experimental.pallas import tpu as pltpu
from jax.sharding import PartitionSpec as P

MESH = pl.DeviceIdType.MESH
OUT = (0, 0), (1, 0)
OUT_NEXT = (0, 0), (1, 0)
BACK = (1, 0), (0, 0)
F32, BF16 = jnp.float32, jnp.bfloat16


def mode_table(count):
    rank = np.arange(count)
    angle = np.pi / (4 * count) * ((2 * rank[:, None] + 1) * (2 * rank[None, :] + 1) % (8 * count))
    table = (np.cos(angle) * np.sqrt(2.0 / count)).astype(np.float32)
    high = table.astype(jnp.bfloat16)
    low = (table - high.astype(np.float32)).astype(jnp.bfloat16)
    return np.stack([high, low])


def split(values):
    high = values.astype(BF16)
    return high, (values - high.astype(F32)).astype(BF16)


def dot(a, b, dims):
    out = None
    for i, j in ((0, 1), (1, 0), (0, 0)):
        term = lax.dot_general(a[i], b[j], (dims, ((), ())), preferred_element_type=F32)
        out = term if out is None else out + term
    return out


NN, NT, TN = ((1,), (0,)), ((1,), (1,)), ((0,), (0,))


def exchanged(tiles):
    tiles = pltpu.roll(tiles, 0, 2, stride=16, stride_axis=1)
    group = lax.broadcasted_iota(jnp.int32, tiles.shape, 2) // 16
    for bit, step in ((1, 7), (2, 6), (4, 4)):
        tiles = jnp.where(group // bit % 2 == 1, pltpu.roll(tiles, step, 1), tiles)
    return pltpu.roll(tiles, 0, 2, stride=16, stride_axis=1)


def kernel(a_ref, hx_ref, h_ref, hb_ref, hc_ref, sx_ref, sy_ref, sz_ref, out_ref,
           send1, recv1, recv2, send3, recv3, recv4, send_sem, recv_sem, own_sem):
    r, c = lax.axis_index("row"), lax.axis_index("col")
    a = r % 8 * 2 + c % 2
    b = r // 8 * 8 + c // 2

    def at_a(t):
        return {"row": b // 8 * 8 + t // 2, "col": b % 8 * 2 + t % 2}

    def at_b(t):
        return {"row": t // 8 * 8 + a // 2, "col": t % 8 * 2 + a % 2}

    barrier = pltpu.get_barrier_semaphore()

    @pl.loop(1, 16)
    def _(i):
        pl.semaphore_signal(barrier, inc=1, device_id=at_a((a + i) % 16), device_id_type=MESH)
        pl.semaphore_signal(barrier, inc=1, device_id=at_b((b + i) % 16), device_id_type=MESH)

    def slot(col):
        return col // 8 * 8 + (8 - col % 8) % 8

    half = a // 8
    near, far = half * 8, (1 - half) * 8

    def refs(k, h, base, mine, t):
        if k == 0:
            return send1.at[:, t], recv1.at[:, mine]
        if k == 1:
            return recv1.at[:, pl.ds(base, 8), pl.ds(t, 1)], recv2.at[:, pl.ds(base, 8), pl.ds(mine, 1)]
        if k == 2:
            return send3.at[:, pl.ds(base, 8), pl.ds(slot(t), 1)], recv3.at[:, pl.ds(base, 8), pl.ds(mine, 1)]
        return recv3.at[:, t], recv4.at[:, mine]

    def own(k, h, side):
        return pltpu.make_async_copy(*refs(k, h, (near, far)[side], *((a, a) if k in (0, 3) else (b, b))),
                                     own_sem.at[k, side, h])

    def start(k, side, h):
        base, rows = (near, far)[side], k in (0, 3)
        mine, at = (a, at_a) if rows else (b, at_b)

        @pl.loop(0 if rows and side else 1, 8 if rows else 16)
        def _(i):
            t = base + (a + i) % 8 if rows else (b + i) % 16
            src, dst = refs(k, h, base, mine, t)
            pltpu.make_async_remote_copy(src, dst, send_sem.at[k, side, h], recv_sem.at[k, side, h],
                                         device_id=at(t), device_id_type=MESH).start()
        if not (rows and side):
            own(k, h, side).start()

    def await_all(k, side, h, sem):
        part = send1.at[:, pl.ds(0, 7 + side)] if k in (0, 3) else send1.at[:, pl.ds(0, 15), pl.ds(0, 8)]
        pltpu.make_async_copy(part, part, sem.at[k, side, h]).wait()

    def finish(k, side, h):
        if k in (1, 2) or not side:
            own(k, h, side).wait()
        await_all(k, side, h, recv_sem)

    hx = hx_ref[0], hx_ref[1]
    table = h_ref[0], h_ref[1]
    backwards = hb_ref[0], hb_ref[1]
    columns = hc_ref[0], hc_ref[1]
    for f in range(2):
        for h in range(2):
            rows = split(a_ref[f, pl.ds(8 * h, 8)].reshape(128, 128))
            send1[h, pl.ds(8 * f, 8)] = dot(hx, rows, NT).reshape(8, 16, 128)
    pl.semaphore_wait(barrier, 30)
    for side, h in OUT:
        start(0, side, h)

    symbol_y = jnp.broadcast_to(sy_ref[...], (256, 256)).T
    symbol = sx_ref[a % 8 * 16 + b] + symbol_y + sz_ref[...]
    scale = lax.rsqrt(symbol)

    for side, h in OUT_NEXT:
        finish(0, side, h)
        start(1, side, h)
    for side, h in OUT_NEXT:
        finish(1, side, h)

    tiles = exchanged(recv2[...].reshape(64, 8, 128)).reshape(2, 8, 2, 2, 8, 128)
    plane = jnp.concatenate(
        [jnp.stack([jnp.stack([tiles[h, :, g, y] for h in range(2)], axis=1) for y in range(2)]).reshape(256, 128)
         for g in range(2)], axis=1
    )
    plane = dot(split(plane), columns, NN)
    plane = dot(backwards, split(plane), NN) * scale
    plane = dot(table, split(plane), NN)
    plane = dot(split(plane), columns, NT).reshape(2, 8, 2, 8, 256)
    for h in range(2):
        part = jnp.stack(
            [jnp.stack([plane[y, :, h, :, 128 * g:128 * (g + 1)] for y in range(2)], axis=1) for g in range(2)], axis=1
        ).reshape(32, 8, 128)
        send3[h] = exchanged(part).reshape(16, 16, 128)
    for side, h in BACK:
        start(2, side, h)
    for side, h in BACK:
        finish(2, side, h)
        start(3, side, h)
    for side, h in BACK:
        finish(3, side, h)
        f = (half, 1 - half)[side]
        for h in range(2):
            rows = split(recv4[h, pl.ds(8 * f, 8)].reshape(128, 128))
            out_ref[f, pl.ds(8 * h, 8)] = dot(rows, hx, TN).reshape(8, 16, 128)
    for k in range(4):
        for side, h in OUT:
            await_all(k, side, h, send_sem)


def shards(tracer, symbol_x, symbol_y, symbol_z):
    values = jnp.transpose(tracer, (0, 2, 3, 1))
    vmem, smem = pl.BlockSpec(memory_space=pltpu.VMEM), pl.BlockSpec(memory_space=pltpu.SMEM)
    table, place = mode_table(256), np.arange(256)
    backwards = place // 8 * 8 + -place % 8
    apart = (place % 128 // 16 * 2 + place // 128) * 16 + place % 16
    block = pltpu.VMEM((2, 16, 16, 128), F32)
    out = pl.pallas_call(
        kernel,
        out_shape=jax.ShapeDtypeStruct(values.shape, F32),
        in_specs=[vmem, vmem, vmem, vmem, vmem, smem, vmem, vmem],
        out_specs=vmem,
        scratch_shapes=[block] * 6 + [pltpu.SemaphoreType.DMA((4, 2, 2))] * 3,
        compiler_params=pltpu.CompilerParams(collective_id=0, has_side_effects=True),
    )(values, jnp.asarray(mode_table(128)), jnp.asarray(table), jnp.asarray(table[:, :, backwards]),
      jnp.asarray(table[:, apart]),
      symbol_x, symbol_y.reshape(1, 256), symbol_z.reshape(1, 256))
    return jnp.transpose(out, (0, 3, 1, 2))


def solution(mesh):
    in_specs = (P("unit", None, "row", "col"), P(), P(), P())
    out_specs = P("unit", None, "row", "col")
    return jax.shard_map(shards, mesh=mesh, in_specs=in_specs, out_specs=out_specs, check_vma=False)
```

```python
import functools

import jax
import jax.numpy as jnp
import numpy as np
from jax import lax
from jax.experimental import pallas as pl
from jax.experimental.pallas import tpu as pltpu
from jax.sharding import PartitionSpec as P

MESH = pl.DeviceIdType.MESH
OUT = (0, 0), (1, 0)
OUT_NEXT = (0, 0), (1, 0)
BACK = (1, 0), (0, 0)
F32, BF16 = jnp.float32, jnp.bfloat16


def mode_table(count):
    rank = np.arange(count)
    angle = np.pi / (4 * count) * ((2 * rank[:, None] + 1) * (2 * rank[None, :] + 1) % (8 * count))
    table = (np.cos(angle) * np.sqrt(2.0 / count)).astype(np.float32)
    high = table.astype(jnp.bfloat16)
    low = (table - high.astype(np.float32)).astype(jnp.bfloat16)
    return np.stack([high, low])


def split(values):
    high = values.astype(BF16)
    return high, (values - high.astype(F32)).astype(BF16)


def dot(a, b, dims):
    out = None
    for i, j in ((0, 1), (1, 0), (0, 0)):
        term = lax.dot_general(a[i], b[j], (dims, ((), ())), preferred_element_type=F32)
        out = term if out is None else out + term
    return out


NN, NT, TN = ((1,), (0,)), ((1,), (1,)), ((0,), (0,))


def exchanged(tiles):
    tiles = pltpu.roll(tiles, 0, 2, stride=16, stride_axis=1)
    group = lax.broadcasted_iota(jnp.int32, tiles.shape, 2) // 16
    for bit, step in ((1, 7), (2, 6), (4, 4)):
        tiles = jnp.where(group // bit % 2 == 1, pltpu.roll(tiles, step, 1), tiles)
    return pltpu.roll(tiles, 0, 2, stride=16, stride_axis=1)


def kernel(a_ref, hx_ref, h_ref, hb_ref, hc_ref, sx_ref, sy_ref, sz_ref, out_ref,
           send1, recv1, recv2, send3, recv3, recv4, send_sem, recv_sem, own_sem):
    r, c = lax.axis_index("row"), lax.axis_index("col")
    a = r % 8 * 2 + c % 2
    b = r // 8 * 8 + c // 2

    def at_a(t):
        return {"row": b // 8 * 8 + t // 2, "col": b % 8 * 2 + t % 2}

    def at_b(t):
        return {"row": t // 8 * 8 + a // 2, "col": t % 8 * 2 + a % 2}

    barrier = pltpu.get_barrier_semaphore()

    @pl.loop(1, 16)
    def _(i):
        pl.semaphore_signal(barrier, inc=1, device_id=at_a((a + i) % 16), device_id_type=MESH)
        pl.semaphore_signal(barrier, inc=1, device_id=at_b((b + i) % 16), device_id_type=MESH)

    def slot(col):
        return col // 8 * 8 + (8 - col % 8) % 8

    half = a // 8
    near, far = half * 8, (1 - half) * 8

    def refs(k, h, base, mine, t):
        if k == 0:
            return send1.at[:, t], recv1.at[:, mine]
        if k == 1:
            return recv1.at[:, pl.ds(base, 8), pl.ds(t, 1)], recv2.at[:, pl.ds(base, 8), pl.ds(mine, 1)]
        if k == 2:
            return send3.at[:, pl.ds(base, 8), pl.ds(slot(t), 1)], recv3.at[:, pl.ds(base, 8), pl.ds(mine, 1)]
        return recv3.at[:, t], recv4.at[:, mine]

    def own(k, h, side):
        return pltpu.make_async_copy(*refs(k, h, (near, far)[side], *((a, a) if k in (0, 3) else (b, b))),
                                     own_sem.at[k, side, h])

    def start(k, side, h):
        base, rows = (near, far)[side], k in (0, 3)
        mine, at = (a, at_a) if rows else (b, at_b)

        @pl.loop(0 if side or not rows else 1, 8 if rows else 15)
        def _(i):
            t = base + (a + i) % 8 if rows else ((b // 8 + 1 + i % 2) % 2) * 8 + (b + 1 + i // 2) % 8
            src, dst = refs(k, h, base, mine, t)
            pltpu.make_async_remote_copy(src, dst, send_sem.at[k, side, h], recv_sem.at[k, side, h],
                                         device_id=at(t), device_id_type=MESH).start()
        if not (rows and side):
            own(k, h, side).start()

    def await_all(k, side, h, sem):
        part = send1.at[:, pl.ds(0, 7 + side)] if k in (0, 3) else send1.at[:, pl.ds(0, 15), pl.ds(0, 8)]
        pltpu.make_async_copy(part, part, sem.at[k, side, h]).wait()

    def finish(k, side, h):
        if k in (1, 2) or not side:
            own(k, h, side).wait()
        await_all(k, side, h, recv_sem)

    hx = hx_ref[0], hx_ref[1]
    table = h_ref[0], h_ref[1]
    backwards = hb_ref[0], hb_ref[1]
    columns = hc_ref[0], hc_ref[1]
    for f in range(2):
        for h in range(2):
            rows = split(a_ref[f, pl.ds(8 * h, 8)].reshape(128, 128))
            send1[h, pl.ds(8 * f, 8)] = dot(hx, rows, NT).reshape(8, 16, 128)
    pl.semaphore_wait(barrier, 30)
    for side, h in OUT:
        start(0, side, h)

    symbol_y = jnp.broadcast_to(sy_ref[...], (256, 256)).T
    symbol = sx_ref[a % 8 * 16 + b] + symbol_y + sz_ref[...]
    scale = lax.rsqrt(symbol)

    for side, h in OUT_NEXT:
        finish(0, side, h)
        start(1, side, h)
    for side, h in OUT_NEXT:
        finish(1, side, h)

    tiles = exchanged(recv2[...].reshape(64, 8, 128)).reshape(2, 8, 2, 2, 8, 128)
    plane = jnp.concatenate(
        [jnp.stack([jnp.stack([tiles[h, :, g, y] for h in range(2)], axis=1) for y in range(2)]).reshape(256, 128)
         for g in range(2)], axis=1
    )
    plane = dot(split(plane), columns, NN)
    plane = dot(backwards, split(plane), NN) * scale
    plane = dot(table, split(plane), NN)
    plane = dot(split(plane), columns, NT).reshape(2, 8, 2, 8, 256)
    for h in range(2):
        part = jnp.stack(
            [jnp.stack([plane[y, :, h, :, 128 * g:128 * (g + 1)] for y in range(2)], axis=1) for g in range(2)], axis=1
        ).reshape(32, 8, 128)
        send3[h] = exchanged(part).reshape(16, 16, 128)
    for side, h in BACK:
        start(2, side, h)
    for side, h in BACK:
        finish(2, side, h)
        start(3, side, h)
    for side, h in BACK:
        finish(3, side, h)
        f = (half, 1 - half)[side]
        for h in range(2):
            rows = split(recv4[h, pl.ds(8 * f, 8)].reshape(128, 128))
            out_ref[f, pl.ds(8 * h, 8)] = dot(rows, hx, TN).reshape(8, 16, 128)
    for k in range(4):
        for side, h in OUT:
            await_all(k, side, h, send_sem)


def shards(tracer, symbol_x, symbol_y, symbol_z):
    values = jnp.transpose(tracer, (0, 2, 3, 1))
    vmem, smem = pl.BlockSpec(memory_space=pltpu.VMEM), pl.BlockSpec(memory_space=pltpu.SMEM)
    table, place = mode_table(256), np.arange(256)
    backwards = place // 8 * 8 + -place % 8
    apart = (place % 128 // 16 * 2 + place // 128) * 16 + place % 16
    block = pltpu.VMEM((2, 16, 16, 128), F32)
    out = pl.pallas_call(
        kernel,
        out_shape=jax.ShapeDtypeStruct(values.shape, F32),
        in_specs=[vmem, vmem, vmem, vmem, vmem, smem, vmem, vmem],
        out_specs=vmem,
        scratch_shapes=[block] * 6 + [pltpu.SemaphoreType.DMA((4, 2, 2))] * 3,
        compiler_params=pltpu.CompilerParams(collective_id=0, has_side_effects=True),
    )(values, jnp.asarray(mode_table(128)), jnp.asarray(table), jnp.asarray(table[:, :, backwards]),
      jnp.asarray(table[:, apart]),
      symbol_x, symbol_y.reshape(1, 256), symbol_z.reshape(1, 256))
    return jnp.transpose(out, (0, 3, 1, 2))


def solution(mesh):
    in_specs = (P("unit", None, "row", "col"), P(), P(), P())
    out_specs = P("unit", None, "row", "col")
    return jax.shard_map(shards, mesh=mesh, in_specs=in_specs, out_specs=out_specs, check_vma=False)
```
